512 devices in a mesh: lvl: 4 (over z_lo), gx: 16 (over y, z_hi), gy: 8 (over x, core).
Axes of the slice: x: 4, y: 4, z: 16 (z_hi: 4, z_lo: 4; z = z_hi * 4 + z_lo), core: 2. Of those that a mesh axis runs over, the one named last changes fastest.
Arguments:
- initial: float32 [256, 256, 256], P('gx', 'gy'), may hold values from -6 to 6
- reaction: float32 [256, 256, 256], P('gx', 'gy'), may hold values from -0.5 to 0
Outputs:
- levels: float32 [4, 256, 256, 256], P('lvl', 'gx', 'gy')
The draws below stay inside these ranges and needn't reach their ends.
All inputs are finite; a program needn't handle non-finite values.
Results may differ from the reference program's by a relative error of at most 0.0001.
Values sent between devices are 32-bit elements; how exact they have to be, the bound alone decides.
A program may use at most 64 MiB of HBM per device.

```python
import jax
import jax.numpy as jnp

NX = 256
NY = 256
NZ = 256
STEPS = 1
KX = 128
KY = 128
KZ = 64
N_LVL = 4


def shard_levels(stream_key, extent, split, low, largest):
    def one(axis_at, blocks):
        heights = jax.random.uniform(jax.random.fold_in(jax.random.fold_in(stream_key, 6), axis_at), (blocks,), jnp.float32, low / len(split), largest / len(split))
        return jnp.repeat(jnp.exp(heights), extent[axis_at] // blocks).reshape((-1,) + (1,) * (len(extent) - axis_at - 1))

    gain = one(*split[0])
    for cut in split[1:]:
        gain = gain * one(*cut)
    return gain


def gaussian(key, extent, spread, bound, pieces=(), dtype=jnp.bfloat16):
    values = spread * jax.random.normal(key, extent, jnp.float32)
    if pieces:
        values = values * shard_levels(key, extent, pieces, -0.22, 0.18)
    return jnp.clip(values, -bound, bound).astype(dtype)


def setup_inputs(seed: int = 0) -> dict:
    streams_of = jax.random.split(jax.random.key(seed), 3)
    initial = gaussian(streams_of[0], (NX, NY, NZ), 1.0, 6.0, ((0, 16), (1, 8)), jnp.float32)
    reaction = jnp.clip(-0.5 + 0.5 * jax.random.uniform(streams_of[1], (NX, NY, NZ), jnp.float32) ** shard_levels(streams_of[1], (NX, NY, NZ), ((0, 16), (1, 8)), -0.2, 0.2), -0.5, 0.0)
    return {"initial": initial, "reaction": reaction}


DIFFUSE = 0.3


def evaluate(grid_field, reaction):
    spectrum = jnp.fft.rfftn(grid_field)
    index_x = (jnp.arange(KX) - KX // 2) % NX
    index_y = (jnp.arange(KY) - KY // 2) % NY
    index_z = jnp.arange(KZ)
    kept = spectrum[index_x][:, index_y][:, :, :KZ]
    wave_x = ((jnp.arange(KX) - KX // 2).astype(jnp.float32) / (NX // 4))[:, None, None]
    wave_y = ((jnp.arange(KY) - KY // 2).astype(jnp.float32) / (NY // 4))[None, :, None]
    wave_z = (jnp.arange(KZ).astype(jnp.float32) / (NZ // 4))[None, None, :]
    factor_real = -DIFFUSE * (wave_x * wave_x + wave_y * wave_y + wave_z * wave_z)
    factor_imag = -(0.3 * wave_x + 0.2 * wave_y + 0.25 * wave_z)
    scaled = kept * (factor_real + 1j * factor_imag)
    filled = jnp.zeros_like(spectrum).at[index_x[:, None, None], index_y[None, :, None], index_z[None, None, :]].set(scaled)
    values = jnp.fft.irfftn(filled, s=(NX, NY, NZ)).astype(jnp.float32)
    return values + reaction * grid_field


def reference(initial, reaction):
    previous = None
    finals = []
    for level_index in range(N_LVL):
        current = initial
        terms = [evaluate(current, reaction)]
        for position in range(STEPS):
            update = current + terms[position]
            if previous is not None:
                update = update + 0.5 * (previous[position + 1] - previous[position])
            current = update
            terms.append(evaluate(current, reaction))
        finals.append(current)
        previous = terms
    return jnp.stack(finals)
```

```python
import functools
import math

import jax
import jax.numpy as jnp
import numpy as np
from jax import lax
from jax.experimental import pallas as pl
from jax.experimental.pallas import tpu as pltpu
from jax.sharding import PartitionSpec as P

CELLS = 256
MODES = 128
DEPTH_MODES = 64
LEVELS = 4
PARTS_X = 16
PARTS_Y = 8
PLANE = LEVELS * PARTS_X
SLAB = CELLS // PLANE
ROWS_Y = CELLS // PARTS_Y
ROWS_X = CELLS // PARTS_X
RING_Z = 16
RING_Y = 4
DIFFUSE = 0.3
NORM = 1.0 / CELLS**3
LANES = 128
MESH = pl.DeviceIdType.MESH
F32 = jnp.float32
BF16 = jnp.bfloat16

Y_OUT, X_OUT, X_BACK, Y_BACK, Y_OUT2, X_OUT2, X_BACK2, BULK, FINAL = range(9)
PHASES = FINAL + LEVELS


def halves(table):
    high = table.astype(BF16)
    low = (table - high.astype(np.float64)).astype(BF16)
    return np.concatenate([high, low], axis=0)


def tables():
    points = np.arange(CELLS)
    step = 2.0 * math.pi / CELLS

    def phase(wave):
        angle = (points[:, None] * wave[None, :] % CELLS) * step
        return np.cos(angle), np.sin(angle)

    wave_z = np.arange(DEPTH_MODES)
    cos_z, sin_z = phase(wave_z)
    per_part = DEPTH_MODES // PARTS_Y

    def parts(real, imag):
        stacked = np.stack([real, imag], axis=1)
        stacked = stacked.reshape(CELLS, 2, PARTS_Y, per_part)
        return stacked.transpose(0, 2, 1, 3).reshape(CELLS, LANES)

    forward_z = parts(cos_z, -sin_z)
    weight = np.where(wave_z == 0, 1.0, 2.0)
    back_z = parts(cos_z * weight, -sin_z * weight).T

    wave = np.arange(MODES) - MODES // 2
    cosine, sine = phase(wave)
    forward_y = np.concatenate([cosine.T, sine.T], axis=0)
    back_y = np.concatenate([cosine, sine], axis=1)
    order = (np.arange(PLANE)[None, :] * SLAB + np.arange(SLAB)[:, None]).reshape(-1)
    forward_x = forward_y[:, order]
    back_x = back_y[order, :]
    return [halves(t) for t in (forward_z, forward_y, forward_x, back_x, back_y, back_z)]


def split(x):
    high = x.astype(BF16)
    return high, (x - high.astype(F32)).astype(BF16)


def dot(a, b):
    return jnp.dot(a, b, preferred_element_type=F32)


def table_times(table, data):
    rows = table.shape[0] // 2
    high, low = split(data)
    first = dot(table[...], high)
    return first[:rows] + first[rows:] + dot(table[:rows, :], low)


def times_table(data, table):
    depth = table.shape[0] // 2
    rows = data.shape[0]
    high, low = split(data)
    first = dot(jnp.concatenate([high, low], axis=0), table[:depth, :])
    return first[:rows] + first[rows:] + dot(high, table[depth:, :])


def lane_index(shape):
    return lax.broadcasted_iota(jnp.int32, shape, 1)


def roll(x, shift):
    return x if shift % LANES == 0 else pltpu.roll(x, shift % LANES, 1)


def turn(x):
    real = (lane_index(x.shape) & 8) == 0
    return jnp.where(real, -roll(x, -8), roll(x, 8))


def swap_groups(mats):
    mats = list(mats)
    group = lane_index(mats[0].shape) // 16
    for bit in (1, 2, 4):
        keep = (group & bit) == 0
        for low in range(8):
            if low & bit:
                continue
            high = low | bit
            a, b = mats[low], mats[high]
            mats[low] = jnp.where(keep, a, roll(b, 16 * bit))
            mats[high] = jnp.where(keep, roll(a, -16 * bit), b)
    return mats


def kernel(
    v_hbm, r_hbm, tz_hbm, ty_hbm, tx_hbm, bx_hbm, by_hbm, bz_hbm, out_hbm,
    v, r, r_all, tz, ty, tx, bx, by, bz,
    factor, carry, y_send, y_recv, x_send, x_recv, b_send, b_recv, u_send, u_recv, f_recv,
    piece_send, piece, load_sem, send_sem, recv_sem,
):
    lvl, gx, gy = lax.axis_index("lvl"), lax.axis_index("gx"), lax.axis_index("gy")
    row_y, high_z = lax.div(gx, 4), lax.rem(gx, 4)
    at_z = high_z * 4 + lvl
    me = row_y * RING_Z + at_z

    def plane_id(y2, z2):
        return {"gx": y2 * 4 + lax.div(z2, 4), "lvl": lax.rem(z2, 4)}

    def over_plane(do):
        def body(k, carried):
            half = lax.div(k + 1, 2)
            dz = 8 + half * (1 - 2 * lax.rem(k, 2))
            z2 = lax.rem(at_z + dz, RING_Z)
            for dy in (2, 1, 3, 0):
                do(lax.rem(row_y + dy, RING_Y), z2)
            return carried

        lax.fori_loop(0, RING_Z - 1, body, 0)
        for dy in (2, 1, 3):
            do(lax.rem(row_y + dy, RING_Y), at_z)

    barrier = pltpu.get_barrier_semaphore()

    def hello(y2, z2):
        pl.semaphore_signal(barrier, inc=1, device_id=plane_id(y2, z2), device_id_type=MESH)

    over_plane(hello)
    for k in range(1, PARTS_Y):
        pl.semaphore_signal(
            barrier, inc=1, device_id={"gy": lax.rem(gy + k, PARTS_Y)}, device_id_type=MESH
        )

    own = pl.ds(lvl * SLAB, SLAB)
    loads = [
        pltpu.make_async_copy(source, target, load_sem.at[i])
        for i, (source, target) in enumerate(
            [
                (v_hbm.at[own], v),
                (r_hbm.at[own], r),
                (tz_hbm, tz),
                (ty_hbm, ty),
                (tx_hbm, tx),
                (bx_hbm, bx),
                (by_hbm, by),
                (bz_hbm, bz),
                (r_hbm, r_all),
            ]
        )
    ]
    for load in loads:
        load.start()

    def remote(source, target, phase, device_id, send_phase=None):
        return pltpu.make_async_remote_copy(
            src_ref=source,
            dst_ref=target,
            send_sem=send_sem.at[phase if send_phase is None else send_phase],
            recv_sem=recv_sem.at[phase],
            device_id=device_id,
            device_id_type=MESH,
        )

    def received(ref, phase):
        remote(ref, ref, phase, {"gy": gy}).wait_recv()

    def sent(ref, phase):
        remote(ref, ref, phase, {"gy": gy}).wait_send()

    def y_exchange(source, target, phase):
        for k in (4, 3, 5, 2, 6, 1, 7):
            other = lax.rem(gy + k, PARTS_Y)
            remote(source.at[other], target.at[gy], phase, {"gy": other}).start()
        target[gy] = source[gy]

    def x_exchange(source, target, phase, shift):
        def chunk_of(y2, z2):
            return y2 * RING_Z + lax.rem(z2 + RING_Z - shift, RING_Z)

        def send(y2, z2):
            remote(source.at[chunk_of(y2, z2)], target.at[me], phase, plane_id(y2, z2)).start()

        over_plane(send)
        target[me] = source[chunk_of(row_y, at_z)]

    shape = (MODES, LANES)
    lane = lane_index(shape)
    wave_x = (lax.broadcasted_iota(jnp.int32, shape, 0) - MODES // 2).astype(F32) / (CELLS // 4)
    wave_y = ((lane // 32 & 1) + 2 * me - MODES // 2).astype(F32) / (CELLS // 4)
    wave_z = ((lane & 7) + 8 * gy).astype(F32) / (CELLS // 4)
    factor[0] = -DIFFUSE * (wave_x * wave_x + wave_y * wave_y + wave_z * wave_z) * NORM
    factor[1] = -(0.3 * wave_x + 0.2 * wave_y + 0.25 * wave_z) * NORM
    edge = (wave_z == 0.0) & ((wave_x == -1.0) | (wave_y == -1.0))
    factor[2] = jnp.where(edge, 0.5 / NORM, 1.0 / NORM)

    def scaled(x):
        return factor[0] * x + factor[1] * turn(x)

    def z_forward(first, second):
        lines = times_table(jnp.concatenate([first, second], axis=0), tz)
        mats = [
            lines[(field * SLAB + i) * ROWS_Y : (field * SLAB + i + 1) * ROWS_Y]
            for i in range(SLAB)
            for field in range(2)
        ]
        for part, mat in enumerate(swap_groups(mats)):
            y_send[part] = mat

    def z_back(mats):
        lines = swap_groups(mats)
        stacked = jnp.concatenate([lines[2 * i + f] for f in range(2) for i in range(SLAB)], axis=0)
        values = times_table(stacked, bz)
        half = SLAB * ROWS_Y
        return values[:half], values[half:]

    def y_forward():
        both = table_times(ty, y_recv[...].reshape(CELLS, LANES))
        lines = both[:MODES] - turn(both[MODES:])
        x_send.reshape(MODES, LANES)[...] = lines

    def x_middle(carried):
        rows = x_recv.reshape(MODES, LANES)
        first = rows[pl.ds(0, PLANE, stride=2), :]
        second = rows[pl.ds(1, PLANE, stride=2), :]
        low = lane_index(first.shape) < 32
        lines = jnp.concatenate(
            [
                jnp.where(low, roll(first, -32 * i), roll(second, 32 - 32 * i))
                for i in range(SLAB)
            ],
            axis=0,
        )
        both = table_times(tx, lines)
        spectrum = both[:MODES] - turn(both[MODES:])
        is_first = (lane & 16) == 0
        if carried:
            spectrum = spectrum + jnp.where(is_first, roll(factor[2] * carry[...], -16), 0.0)
        rate = scaled(spectrum)
        rate = jnp.where(is_first, rate, scaled(roll(factor[2] * rate, 16) + spectrum))
        if not carried:
            carry[...] = rate
        lines = table_times(bx, jnp.concatenate([rate, turn(rate)], axis=0))
        group = lane_index((PLANE, LANES)) // 32
        target = b_send.reshape(MODES, LANES)
        for ky in range(2):
            out = None
            for i in range(SLAB):
                piece_i = roll(lines[i * PLANE : (i + 1) * PLANE], 32 * (i - ky))
                out = piece_i if out is None else jnp.where(group == i, piece_i, out)
            target[pl.ds(ky, PLANE, stride=2), :] = out

    def y_back():
        lines = b_recv.reshape(MODES, LANES)[...]
        cells = table_times(by, jnp.concatenate([lines, turn(lines)], axis=0))
        u_send[...] = cells.reshape(PARTS_Y, ROWS_Y, LANES)

    for i in range(3):
        loads[i].wait()
    start = v[...].reshape(SLAB * ROWS_Y, CELLS)
    react = r[...].reshape(SLAB * ROWS_Y, CELLS)
    z_forward(start, react * start)
    for i in range(3, 8):
        loads[i].wait()
    pl.semaphore_wait(barrier, PLANE - 1 + PARTS_Y - 1)

    others_y = pl.ds(0, PARTS_Y - 1)
    others_x = pl.ds(0, PLANE - 1)
    y_exchange(y_send, y_recv, Y_OUT)
    received(y_recv.at[others_y], Y_OUT)
    y_forward()
    x_exchange(x_send, x_recv, X_OUT, 0)
    received(x_recv.at[others_x], X_OUT)
    x_middle(False)
    x_exchange(b_send, b_recv, X_BACK, 0)
    received(b_recv.at[others_x], X_BACK)
    y_back()
    sent(y_send.at[others_y], Y_OUT)
    y_exchange(u_send, u_recv, Y_BACK)
    received(u_recv.at[others_y], Y_BACK)
    smooth, smooth_rate = z_back([u_recv[part] for part in range(PARTS_Y)])
    rate1 = smooth + react * start
    rate2 = smooth_rate + react * rate1
    z_forward(react * rate1, react * rate2)

    sent(x_send.at[others_x], X_OUT)
    sent(b_send.at[others_x], X_BACK)
    y_exchange(y_send, y_recv, Y_OUT2)
    known = start + rate1
    piece_send[0] = known.reshape(SLAB, ROWS_Y, CELLS)
    known = known + 0.5 * rate2
    piece_send[1] = known.reshape(SLAB, ROWS_Y, CELLS)
    known = known + 0.25 * (react * rate2)
    piece_send[2] = known.reshape(SLAB, ROWS_Y, CELLS)
    known = known + 0.125 * (react * (react * rate2))
    piece_send[3] = known.reshape(SLAB, ROWS_Y, CELLS)
    for k in range(1, LEVELS):
        other = lax.rem(lvl + k, LEVELS)
        remote(piece_send.at[other], piece.at[own], BULK, {"lvl": other}).start()
    piece[own] = piece_send[lvl]

    received(y_recv.at[others_y], Y_OUT2)
    y_forward()
    x_exchange(x_send, x_recv, X_OUT2, 0)
    received(x_recv.at[others_x], X_OUT2)
    x_middle(True)
    x_exchange(b_send, b_recv, X_BACK2, 1)
    received(b_recv.at[others_x], X_BACK2)
    sent(u_send.at[others_y], Y_BACK)
    y_back()

    before = lax.rem(at_z + RING_Z - 1, RING_Z)
    slab, block = lax.rem(before, 4), row_y * 4 + lax.div(before, 4)

    def last(level, k):
        other = lax.rem(gy + k, PARTS_Y)
        remote(
            u_send.at[other],
            f_recv.at[slab, gy],
            FINAL + slab,
            {"lvl": level, "gx": block, "gy": other},
            FINAL + level,
        ).start()

    for k in (4, 3, 5, 2, 6, 1, 7):
        for level in (3, 2):
            last(level, k)
    for level in (3, 2):
        @pl.when(lvl != level)
        def _(level=level):
            last(level, 0)

        @pl.when(lvl == level)
        def _():
            f_recv[slab, gy] = u_send[gy]

    loads[8].wait()
    received(piece.at[pl.ds(0, ROWS_X - SLAB)], BULK)

    @pl.when(lvl >= 2)
    def _():
        last_weight = jnp.where(lvl == 3, 0.125, 0.0)
        for t in range(LEVELS):
            @pl.when(lvl - 1 != t)
            def _(t=t):
                received(f_recv.at[t], FINAL + t)

            @pl.when(lvl - 1 == t)
            def _(t=t):
                received(f_recv.at[t, others_y], FINAL + t)

            first, second = z_back([f_recv[t, part] for part in range(PARTS_Y)])
            at = pl.ds(t * SLAB, SLAB)
            first = first.reshape(SLAB, ROWS_Y, CELLS)
            second = second.reshape(SLAB, ROWS_Y, CELLS)
            piece[at] = piece[at] + (0.25 + last_weight * r_all[at]) * first + last_weight * second

    result = pltpu.make_async_copy(piece, out_hbm.at[0], load_sem.at[0])
    result.start()

    sent(y_send.at[others_y], Y_OUT2)
    sent(x_send.at[others_x], X_OUT2)
    sent(b_send.at[others_x], X_BACK2)
    sent(piece_send.at[pl.ds(0, 3)], BULK)
    for level in (3, 2):
        @pl.when(lvl != level)
        def _(level=level):
            sent(u_send, FINAL + level)

        @pl.when(lvl == level)
        def _(level=level):
            sent(u_send.at[others_y], FINAL + level)

    result.wait()


def solution(mesh):
    constants = tables()

    def shards(initial, reaction):
        rows = (SLAB, ROWS_Y, CELLS)
        block = (ROWS_X, ROWS_Y, CELLS)
        lines = (PARTS_Y, ROWS_Y, LANES)
        chunks = (PLANE, 2, LANES)
        vmem = pltpu.VMEM
        return pl.pallas_call(
            kernel,
            out_shape=jax.ShapeDtypeStruct((1, *block), F32),
            in_specs=[pl.BlockSpec(memory_space=pl.ANY)] * 8,
            out_specs=pl.BlockSpec(memory_space=pl.ANY),
            scratch_shapes=[
                vmem(rows, F32),
                vmem(rows, F32),
                vmem(block, F32),
                *[vmem(t.shape, BF16) for t in constants],
                vmem((3, MODES, LANES), F32),
                vmem((MODES, LANES), F32),
                vmem(lines, F32),
                vmem(lines, F32),
                vmem(chunks, F32),
                vmem(chunks, F32),
                vmem(chunks, F32),
                vmem(chunks, F32),
                vmem(lines, F32),
                vmem(lines, F32),
                vmem((LEVELS, *lines), F32),
                vmem((LEVELS, *rows), F32),
                vmem(block, F32),
                pltpu.SemaphoreType.DMA((9,)),
                pltpu.SemaphoreType.DMA((PHASES,)),
                pltpu.SemaphoreType.DMA((PHASES,)),
            ],
            compiler_params=pltpu.CompilerParams(collective_id=0, has_side_effects=True),
        )(initial, reaction, *[jnp.asarray(t) for t in constants])

    in_specs = (P("gx", "gy", None), P("gx", "gy", None))
    out_specs = P("lvl", "gx", "gy", None)
    return jax.shard_map(shards, mesh=mesh, in_specs=in_specs, out_specs=out_specs, check_vma=False)
```

```python
import functools
import math

import jax
import jax.numpy as jnp
import numpy as np
from jax import lax
from jax.experimental import pallas as pl
from jax.experimental.pallas import tpu as pltpu
from jax.sharding import PartitionSpec as P

CELLS = 256
MODES = 128
DEPTH_MODES = 64
LEVELS = 4
PARTS_X = 16
PARTS_Y = 8
PLANE = LEVELS * PARTS_X
SLAB = CELLS // PLANE
PAIRS = PLANE // 2
LINES_Y = MODES // PAIRS
ROWS_Y = CELLS // PARTS_Y
ROWS_X = CELLS // PARTS_X
RING_Z = 16
RING_Y = 4
DIFFUSE = 0.3
NORM = 1.0 / CELLS**3
LANES = 128
MESH = pl.DeviceIdType.MESH
F32 = jnp.float32
BF16 = jnp.bfloat16

Y_OUT, X_OUT, X_BACK, Y_BACK, Y_OUT2, X_OUT2, X_BACK2, BULK, FINAL = range(9)
PHASES = FINAL + LEVELS


def halves(table):
    high = table.astype(BF16)
    low = (table - high.astype(np.float64)).astype(BF16)
    return np.concatenate([high, low], axis=0)


def tables():
    points = np.arange(CELLS)
    step = 2.0 * math.pi / CELLS

    def phase(wave):
        angle = (points[:, None] * wave[None, :] % CELLS) * step
        return np.cos(angle), np.sin(angle)

    wave_z = np.arange(DEPTH_MODES)
    cos_z, sin_z = phase(wave_z)
    per_part = DEPTH_MODES // PARTS_Y

    def parts(real, imag):
        stacked = np.stack([real, imag], axis=1)
        stacked = stacked.reshape(CELLS, 2, PARTS_Y, per_part)
        return stacked.transpose(0, 2, 1, 3).reshape(CELLS, LANES)

    forward_z = parts(cos_z, -sin_z)
    weight = np.where(wave_z == 0, 1.0, 2.0)
    back_z = parts(cos_z * weight, -sin_z * weight).T

    wave = np.arange(MODES) - MODES // 2
    cosine, sine = phase(wave)
    forward_y = np.concatenate([cosine.T, sine.T], axis=0)
    back_y = np.concatenate([cosine, sine], axis=1)
    order = (np.arange(PLANE)[None, :] * SLAB + np.arange(SLAB)[:, None]).reshape(-1)
    forward_x = forward_y[:, order]
    back_x = back_y[order, :]
    return [halves(t) for t in (forward_z, forward_y, forward_x, back_x, back_y, back_z)]


def split(x):
    high = x.astype(BF16)
    return high, (x - high.astype(F32)).astype(BF16)


def dot(a, b):
    return jnp.dot(a, b, preferred_element_type=F32)


def table_times(table, data):
    rows = table.shape[0] // 2
    high, low = split(data)
    first = dot(table[...], high)
    return first[:rows] + first[rows:] + dot(table[:rows, :], low)


def times_table(data, table):
    depth = table.shape[0] // 2
    rows = data.shape[0]
    high, low = split(data)
    first = dot(jnp.concatenate([high, low], axis=0), table[:depth, :])
    return first[:rows] + first[rows:] + dot(high, table[depth:, :])


def lane_index(shape):
    return lax.broadcasted_iota(jnp.int32, shape, 1)


def roll(x, shift):
    return x if shift % LANES == 0 else pltpu.roll(x, shift % LANES, 1)


def turn(x):
    real = (lane_index(x.shape) & 8) == 0
    return jnp.where(real, -roll(x, -8), roll(x, 8))


def swap_groups(mats):
    mats = list(mats)
    count = len(mats)
    width = LANES // count
    group = lane_index(mats[0].shape) // width
    bit = 1
    while bit < count:
        keep = (group & bit) == 0
        for low in range(count):
            if low & bit:
                continue
            high = low | bit
            a, b = mats[low], mats[high]
            mats[low] = jnp.where(keep, a, roll(b, width * bit))
            mats[high] = jnp.where(keep, roll(a, -width * bit), b)
        bit *= 2
    return mats


def hops(dy, dz):
    return min(dy, RING_Y - dy) + min(dz, RING_Z - dz)


def offsets():
    every = [(dy, dz) for dz in range(RING_Z) for dy in range(RING_Y) if (dy, dz) != (0, 0)]
    every.sort(key=lambda o: -hops(*o))
    near = []
    for dy, dz in every:
        opposite = ((dy + 2) % RING_Y, (dz + 8) % RING_Z)
        if opposite not in near and hops(dy, dz) <= hops(*opposite):
            near.append((dy, dz))
    return every, near


def kernel(
    v_hbm, r_hbm, tz_hbm, ty_hbm, tx_hbm, bx_hbm, by_hbm, bz_hbm, piece,
    v, r, r_all, tz, ty, tx, bx, by, bz,
    factor, carry, y_send, y_recv, x_send, x_recv1, x_recv2, b_send, b_recv, u_send, u_recv, f_recv,
    piece_send, load_sem, send_sem, recv_sem, ready,
):
    lvl, gx, gy = lax.axis_index("lvl"), lax.axis_index("gx"), lax.axis_index("gy")
    row_y, high_z = lax.div(gx, 4), lax.rem(gx, 4)
    at_z = high_z * 4 + lvl
    me = row_y * RING_Z + at_z

    pair = lax.rem(row_y, 2) * RING_Z + lax.rem(at_z + 8 * lax.div(row_y, 2), RING_Z)

    def place(dy, dz):
        return lax.rem(row_y + dy, RING_Y), lax.rem(at_z + dz, RING_Z)

    def plane_id(y2, z2):
        return {"gx": y2 * 4 + lax.div(z2, 4), "lvl": lax.rem(z2, 4)}

    every, near = offsets()

    own = pl.ds(lvl * SLAB, SLAB)
    loads = [
        pltpu.make_async_copy(source, target, load_sem.at[i])
        for i, (source, target) in enumerate(
            [
                (v_hbm.at[own], v),
                (r_hbm.at[own], r),
                (tz_hbm, tz),
                (ty_hbm, ty),
                (tx_hbm, tx),
                (bx_hbm, bx),
                (by_hbm, by),
                (bz_hbm, bz),
                (r_hbm, r_all),
            ]
        )
    ]
    for load in loads[:3]:
        load.start()

    barrier = pltpu.get_barrier_semaphore()
    heard = 0
    for dy, dz in every:
        if min(dz, RING_Z - dz) <= 4:
            pl.semaphore_signal(
                barrier, inc=1, device_id=plane_id(*place(dy, dz)), device_id_type=MESH
            )
            heard += 1
    for k in (4, 3, 5, 2, 6, 1, 7):
        pl.semaphore_signal(
            barrier, inc=1, device_id={"gy": lax.rem(gy + k, PARTS_Y)}, device_id_type=MESH
        )
        heard += 1
    for load in loads[3:]:
        load.start()

    def remote(source, target, phase, device_id, send_phase=None):
        return pltpu.make_async_remote_copy(
            src_ref=source,
            dst_ref=target,
            send_sem=send_sem.at[phase if send_phase is None else send_phase],
            recv_sem=recv_sem.at[phase],
            device_id=device_id,
            device_id_type=MESH,
        )

    def received(ref, phase):
        remote(ref, ref, phase, {"gy": gy}).wait_recv()

    def sent(ref, phase):
        remote(ref, ref, phase, {"gy": gy}).wait_send()

    def y_exchange(source, target, phase):
        for k in (4, 3, 5, 2, 6, 1, 7):
            other = lax.rem(gy + k, PARTS_Y)
            remote(source.at[other], target.at[gy], phase, {"gy": other}).start()
        target[gy] = source[gy]

    def x_exchange(x_recv, phase):
        def send(y2, z2):
            chunk = lax.rem(y2, 2) * RING_Z + lax.rem(z2 + 8 * lax.div(y2, 2), RING_Z)
            remote(x_send.at[chunk], x_recv.at[me], phase, plane_id(y2, z2)).start()

        for dy, dz in every:
            send(*place(dy, dz))
        x_recv[me] = x_send[pair]

    def x_return(phase, shift):
        def chunk_of(y2, z2):
            return y2 * RING_Z + lax.rem(z2 + RING_Z - shift, RING_Z)

        for dy, dz in near:
            y2, z2 = place(dy, dz)
            remote(b_send.at[chunk_of(y2, z2)], b_recv.at[pair], phase, plane_id(y2, z2)).start()
        b_recv[pair] = b_send[chunk_of(row_y, at_z)]

    shape = (MODES, LANES)
    lane = lane_index(shape)
    wave_x = (lax.broadcasted_iota(jnp.int32, shape, 0) - MODES // 2).astype(F32) / (CELLS // 4)
    wave_y = (lane // 32 + LINES_Y * pair - MODES // 2).astype(F32) / (CELLS // 4)
    wave_z = ((lane & 7) + 8 * gy).astype(F32) / (CELLS // 4)
    factor[0] = -DIFFUSE * (wave_x * wave_x + wave_y * wave_y + wave_z * wave_z) * NORM
    factor[1] = -(0.3 * wave_x + 0.2 * wave_y + 0.25 * wave_z) * NORM
    edge = (wave_z == 0.0) & ((wave_x == -1.0) | (wave_y == -1.0))
    factor[2] = jnp.where(edge, 0.5 / NORM, 1.0 / NORM)

    def scaled(x):
        return factor[0] * x + factor[1] * turn(x)

    def z_forward(first, second):
        lines = times_table(jnp.concatenate([first, second], axis=0), tz)
        mats = [
            lines[(field * SLAB + i) * ROWS_Y : (field * SLAB + i + 1) * ROWS_Y]
            for i in range(SLAB)
            for field in range(2)
        ]
        for part, mat in enumerate(swap_groups(mats)):
            y_send[part] = mat

    def z_back(mats):
        lines = swap_groups(mats)
        stacked = jnp.concatenate([lines[2 * i + f] for f in range(2) for i in range(SLAB)], axis=0)
        values = times_table(stacked, bz)
        half = SLAB * ROWS_Y
        return values[:half], values[half:]

    def y_forward():
        both = table_times(ty, y_recv[...].reshape(CELLS, LANES))
        lines = both[:MODES] - turn(both[MODES:])
        x_send.reshape(MODES, LANES)[...] = lines

    def x_middle(x_recv, carried):
        rows = x_recv.reshape(CELLS, LANES)
        mats = [rows[pl.ds(ky, PLANE, stride=LINES_Y), :] for ky in range(LINES_Y)]
        lines = jnp.concatenate(swap_groups(mats), axis=0)
        both = table_times(tx, lines)
        spectrum = both[:MODES] - turn(both[MODES:])
        is_first = (lane & 16) == 0
        if carried:
            spectrum = spectrum + jnp.where(is_first, roll(factor[2] * carry[...], -16), 0.0)
        rate = scaled(spectrum)
        rate = jnp.where(is_first, rate, scaled(roll(factor[2] * rate, 16) + spectrum))
        if not carried:
            carry[...] = rate
        lines = table_times(bx, jnp.concatenate([rate, turn(rate)], axis=0))
        target = b_send.reshape(CELLS, LANES)
        mats = [lines[i * PLANE : (i + 1) * PLANE] for i in range(SLAB)]
        for ky, mat in enumerate(swap_groups(mats)):
            target[pl.ds(ky, PLANE, stride=LINES_Y), :] = mat

    def y_back():
        lines = b_recv.reshape(MODES, LANES)[...]
        cells = table_times(by, jnp.concatenate([lines, turn(lines)], axis=0))
        u_send[...] = cells.reshape(PARTS_Y, ROWS_Y, LANES)

    for i in range(3):
        loads[i].wait()
    start = v[...].reshape(SLAB * ROWS_Y, CELLS)
    react = r[...].reshape(SLAB * ROWS_Y, CELLS)
    z_forward(start, react * start)
    for i in range(3, 8):
        loads[i].wait()
    pl.semaphore_wait(barrier, heard)
    for dz in (4, RING_Z - 4):
        pl.semaphore_signal(ready, inc=1, device_id=plane_id(*place(0, dz)), device_id_type=MESH)

    others_y = pl.ds(0, PARTS_Y - 1)
    others_x = pl.ds(0, PLANE - 1)
    others_b = pl.ds(0, PAIRS - 1)
    y_exchange(y_send, y_recv, Y_OUT)
    received(y_recv.at[others_y], Y_OUT)
    y_forward()
    pl.semaphore_wait(ready, 2)
    x_exchange(x_recv1, X_OUT)
    received(x_recv1.at[others_x], X_OUT)
    x_middle(x_recv1, False)
    x_return(X_BACK, 0)
    received(b_recv.at[others_b], X_BACK)
    y_back()
    sent(y_send.at[others_y], Y_OUT)
    y_exchange(u_send, u_recv, Y_BACK)
    received(u_recv.at[others_y], Y_BACK)
    smooth, smooth_rate = z_back([u_recv[part] for part in range(PARTS_Y)])
    rate1 = smooth + react * start
    rate2 = smooth_rate + react * rate1
    z_forward(react * rate1, react * rate2)

    sent(x_recv1.at[others_x], X_OUT)
    sent(b_send.at[others_b], X_BACK)
    y_exchange(y_send, y_recv, Y_OUT2)
    known = start + rate1
    piece_send[0] = known.reshape(SLAB, ROWS_Y, CELLS)
    known = known + 0.5 * rate2
    piece_send[1] = known.reshape(SLAB, ROWS_Y, CELLS)
    known = known + 0.25 * (react * rate2)
    piece_send[2] = known.reshape(SLAB, ROWS_Y, CELLS)
    known = known + 0.125 * (react * (react * rate2))
    piece_send[3] = known.reshape(SLAB, ROWS_Y, CELLS)

    def send_pieces(first, last):
        for row in range(first, last):
            for k in range(1, LEVELS):
                other = lax.rem(lvl + k, LEVELS)
                target = piece.at[lvl * SLAB + row]
                remote(piece_send.at[other, row], target, BULK, {"lvl": other}).start()

    send_pieces(0, 1)
    piece[own] = piece_send[lvl]

    received(y_recv.at[others_y], Y_OUT2)
    y_forward()
    x_exchange(x_recv2, X_OUT2)
    send_pieces(1, 2)
    received(x_recv2.at[others_x], X_OUT2)
    send_pieces(2, 3)
    x_middle(x_recv2, True)
    x_return(X_BACK2, 1)
    send_pieces(3, 4)
    received(b_recv.at[others_b], X_BACK2)
    sent(u_send.at[others_y], Y_BACK)
    y_back()

    before = lax.rem(at_z + RING_Z - 1, RING_Z)
    slab, block = lax.rem(before, 4), row_y * 4 + lax.div(before, 4)

    def last(level, k):
        other = lax.rem(gy + k, PARTS_Y)
        remote(
            u_send.at[other],
            f_recv.at[slab, gy],
            FINAL + slab,
            {"lvl": level, "gx": block, "gy": other},
            FINAL + level,
        ).start()

    for k in (4, 3, 5, 2, 6, 1, 7):
        for level in (3, 2):
            last(level, k)
    for level in (3, 2):
        @pl.when(lvl != level)
        def _(level=level):
            last(level, 0)

        @pl.when(lvl == level)
        def _():
            f_recv[slab, gy] = u_send[gy]

    loads[8].wait()
    received(piece.at[pl.ds(0, ROWS_X - SLAB)], BULK)

    @pl.when(lvl >= 2)
    def _():
        last_weight = jnp.where(lvl == 3, 0.125, 0.0)
        for t in range(LEVELS):
            @pl.when(lvl - 1 != t)
            def _(t=t):
                received(f_recv.at[t], FINAL + t)

            @pl.when(lvl - 1 == t)
            def _(t=t):
                received(f_recv.at[t, others_y], FINAL + t)

            first, second = z_back([f_recv[t, part] for part in range(PARTS_Y)])
            at = pl.ds(t * SLAB, SLAB)
            first = first.reshape(SLAB, ROWS_Y, CELLS)
            second = second.reshape(SLAB, ROWS_Y, CELLS)
            piece[at] = piece[at] + (0.25 + last_weight * r_all[at]) * first + last_weight * second


    sent(y_send.at[others_y], Y_OUT2)
    sent(x_recv2.at[others_x], X_OUT2)
    sent(b_send.at[others_b], X_BACK2)
    sent(piece_send.at[pl.ds(0, 3)], BULK)
    for level in (3, 2):
        @pl.when(lvl != level)
        def _(level=level):
            sent(u_send, FINAL + level)

        @pl.when(lvl == level)
        def _(level=level):
            sent(u_send.at[others_y], FINAL + level)


def solution(mesh):
    constants = tables()

    def shards(initial, reaction):
        rows = (SLAB, ROWS_Y, CELLS)
        block = (ROWS_X, ROWS_Y, CELLS)
        lines = (PARTS_Y, ROWS_Y, LANES)
        chunks = (PLANE, LINES_Y, LANES)
        half_chunks = (PAIRS, LINES_Y, LANES)
        vmem = pltpu.VMEM
        result = pl.pallas_call(
            kernel,
            out_shape=pltpu.VMEM(block, F32),
            in_specs=[pl.BlockSpec(memory_space=pl.ANY)] * 8,
            out_specs=pl.BlockSpec(memory_space=pltpu.VMEM),
            scratch_shapes=[
                vmem(rows, F32),
                vmem(rows, F32),
                vmem(block, F32),
                *[vmem(t.shape, BF16) for t in constants],
                vmem((3, MODES, LANES), F32),
                vmem((MODES, LANES), F32),
                vmem(lines, F32),
                vmem(lines, F32),
                vmem(half_chunks, F32),
                vmem(chunks, F32),
                vmem(chunks, F32),
                vmem(chunks, F32),
                vmem(half_chunks, F32),
                vmem(lines, F32),
                vmem(lines, F32),
                vmem((LEVELS, *lines), F32),
                vmem((LEVELS, *rows), F32),
                pltpu.SemaphoreType.DMA((9,)),
                pltpu.SemaphoreType.DMA((PHASES,)),
                pltpu.SemaphoreType.DMA((PHASES,)),
                pltpu.SemaphoreType.REGULAR,
            ],
            compiler_params=pltpu.CompilerParams(collective_id=0, has_side_effects=True),
        )(initial, reaction, *[jnp.asarray(t) for t in constants])
        return result[None]

    in_specs = (P("gx", "gy", None), P("gx", "gy", None))
    out_specs = P("lvl", "gx", "gy", None)
    return jax.shard_map(shards, mesh=mesh, in_specs=in_specs, out_specs=out_specs, check_vma=False)
```

```python
import functools
import math

import jax
import jax.numpy as jnp
import numpy as np
from jax import lax
from jax.experimental import pallas as pl
from jax.experimental.pallas import tpu as pltpu
from jax.sharding import PartitionSpec as P

CELLS = 256
MODES = 128
DEPTH_MODES = 64
LEVELS = 4
PARTS_X = 16
PARTS_Y = 8
PLANE = LEVELS * PARTS_X
SLAB = CELLS // PLANE
PAIRS = PLANE // 2
LINES_Y = MODES // PAIRS
ROWS_Y = CELLS // PARTS_Y
ROWS_X = CELLS // PARTS_X
RING_Z = 16
RING_Y = 4
DIFFUSE = 0.3
NORM = 1.0 / CELLS**3
LANES = 128
MESH = pl.DeviceIdType.MESH
F32 = jnp.float32
BF16 = jnp.bfloat16

Y_OUT, X_OUT, X_BACK, Y_BACK, Y_OUT2, X_OUT2, X_BACK2, BULK, FINAL = range(9)
PHASES = FINAL + LEVELS
CUTS = ((1, 2, 5, 8), (2, 4, 8, 8))


def halves(table):
    high = table.astype(BF16)
    low = (table - high.astype(np.float64)).astype(BF16)
    return np.concatenate([high, low], axis=0)


def tables():
    points = np.arange(CELLS)
    step = 2.0 * math.pi / CELLS

    def phase(wave):
        angle = (points[:, None] * wave[None, :] % CELLS) * step
        return np.cos(angle), np.sin(angle)

    wave_z = np.arange(DEPTH_MODES)
    cos_z, sin_z = phase(wave_z)
    per_part = DEPTH_MODES // PARTS_Y

    def parts(real, imag):
        stacked = np.stack([real, imag], axis=1)
        stacked = stacked.reshape(CELLS, 2, PARTS_Y, per_part)
        return stacked.transpose(0, 2, 1, 3).reshape(CELLS, LANES)

    forward_z = parts(cos_z, -sin_z)
    weight = np.where(wave_z == 0, 1.0, 2.0)
    back_z = parts(cos_z * weight, -sin_z * weight).T

    wave = np.arange(MODES) - MODES // 2
    cosine, sine = phase(wave)
    forward_y = np.concatenate([cosine.T, sine.T], axis=0)
    back_y = np.concatenate([cosine, sine], axis=1)
    order = (np.arange(PLANE)[None, :] * SLAB + np.arange(SLAB)[:, None]).reshape(-1)
    forward_x = forward_y[:, order]
    back_x = back_y[order, :]
    return [halves(t) for t in (forward_z, forward_y, forward_x, back_x, back_y, back_z)]


def split(x):
    high = x.astype(BF16)
    return high, (x - high.astype(F32)).astype(BF16)


def dot(a, b):
    return jnp.dot(a, b, preferred_element_type=F32)


def table_times(table, data):
    rows = table.shape[0] // 2
    high, low = split(data)
    first = dot(table[...], high)
    return first[:rows] + first[rows:] + dot(table[:rows, :], low)


def times_table(data, table):
    depth = table.shape[0] // 2
    rows = data.shape[0]
    high, low = split(data)
    first = dot(jnp.concatenate([high, low], axis=0), table[:depth, :])
    return first[:rows] + first[rows:] + dot(high, table[depth:, :])


def lane_index(shape):
    return lax.broadcasted_iota(jnp.int32, shape, 1)


def roll(x, shift):
    return x if shift % LANES == 0 else pltpu.roll(x, shift % LANES, 1)


def turn(x):
    real = (lane_index(x.shape) & 8) == 0
    return jnp.where(real, -roll(x, -8), roll(x, 8))


def swap_groups(mats):
    mats = list(mats)
    count = len(mats)
    width = LANES // count
    group = lane_index(mats[0].shape) // width
    bit = 1
    while bit < count:
        keep = (group & bit) == 0
        for low in range(count):
            if low & bit:
                continue
            high = low | bit
            a, b = mats[low], mats[high]
            mats[low] = jnp.where(keep, a, roll(b, width * bit))
            mats[high] = jnp.where(keep, roll(a, -width * bit), b)
        bit *= 2
    return mats


def hops(dy, dz):
    return min(dy, RING_Y - dy) + min(dz, RING_Z - dz)


def offsets():
    every = [(dy, dz) for dz in range(RING_Z) for dy in range(RING_Y) if (dy, dz) != (0, 0)]
    every.sort(key=lambda o: -hops(*o))
    near = []
    for dy, dz in every:
        opposite = ((dy + 2) % RING_Y, (dz + 8) % RING_Z)
        if opposite not in near and hops(dy, dz) <= hops(*opposite):
            near.append((dy, dz))
    return every, near


def kernel(
    v_hbm, r_hbm, tz_hbm, ty_hbm, tx_hbm, bx_hbm, by_hbm, bz_hbm, piece,
    v, r, r_all, tz, ty, tx, bx, by, bz,
    factor, carry, y_send, y_recv, x_send, x_recv1, x_recv2, b_send, b_recv, u_send, u_recv, f_recv,
    piece_send, load_sem, send_sem, recv_sem, ready,
):
    lvl, gx, gy = lax.axis_index("lvl"), lax.axis_index("gx"), lax.axis_index("gy")
    row_y, high_z = lax.div(gx, 4), lax.rem(gx, 4)
    at_z = high_z * 4 + lvl
    me = row_y * RING_Z + at_z

    pair = lax.rem(row_y, 2) * RING_Z + lax.rem(at_z + 8 * lax.div(row_y, 2), RING_Z)

    def place(dy, dz):
        return lax.rem(row_y + dy, RING_Y), lax.rem(at_z + dz, RING_Z)

    def plane_id(y2, z2):
        return {"gx": y2 * 4 + lax.div(z2, 4), "lvl": lax.rem(z2, 4)}

    every, near = offsets()

    own = pl.ds(lvl * SLAB, SLAB)
    loads = [
        pltpu.make_async_copy(source, target, load_sem.at[i])
        for i, (source, target) in enumerate(
            [
                (v_hbm.at[own], v),
                (r_hbm.at[own], r),
                (tz_hbm, tz),
                (ty_hbm, ty),
                (tx_hbm, tx),
                (bx_hbm, bx),
                (by_hbm, by),
                (bz_hbm, bz),
                (r_hbm, r_all),
            ]
        )
    ]
    for load in loads[:3]:
        load.start()

    barrier = pltpu.get_barrier_semaphore()
    heard = 0
    for dy, dz in every:
        if min(dz, RING_Z - dz) <= 4 and dy != 2:
            pl.semaphore_signal(
                barrier, inc=1, device_id=plane_id(*place(dy, dz)), device_id_type=MESH
            )
            heard += 1
    for k in (4, 3, 5, 2, 6, 1, 7):
        pl.semaphore_signal(
            barrier, inc=1, device_id={"gy": lax.rem(gy + k, PARTS_Y)}, device_id_type=MESH
        )
        heard += 1
    for load in loads[3:]:
        load.start()

    def remote(source, target, phase, device_id, send_phase=None):
        return pltpu.make_async_remote_copy(
            src_ref=source,
            dst_ref=target,
            send_sem=send_sem.at[phase if send_phase is None else send_phase],
            recv_sem=recv_sem.at[phase],
            device_id=device_id,
            device_id_type=MESH,
        )

    def received(ref, phase):
        remote(ref, ref, phase, {"gy": gy}).wait_recv()

    def sent(ref, phase):
        remote(ref, ref, phase, {"gy": gy}).wait_send()

    def y_exchange(source, target, phase):
        for k in (4, 3, 5, 2, 6, 1, 7):
            other = lax.rem(gy + k, PARTS_Y)
            remote(source.at[other], target.at[gy], phase, {"gy": other}).start()
        target[gy] = source[gy]

    def x_exchange(x_recv, phase):
        def send(y2, z2):
            chunk = lax.rem(y2, 2) * RING_Z + lax.rem(z2 + 8 * lax.div(y2, 2), RING_Z)
            remote(x_send.at[chunk], x_recv.at[me], phase, plane_id(y2, z2)).start()

        for dy, dz in every:
            send(*place(dy, dz))
        x_recv[me] = x_send[pair]

    def x_return(phase, shift):
        def chunk_of(y2, z2):
            return y2 * RING_Z + lax.rem(z2 + RING_Z - shift, RING_Z)

        for dy, dz in near:
            y2, z2 = place(dy, dz)
            remote(b_send.at[chunk_of(y2, z2)], b_recv.at[pair], phase, plane_id(y2, z2)).start()
        b_recv[pair] = b_send[chunk_of(row_y, at_z)]

    def prepare_factor():
        shape = (MODES, LANES)
        lane = lane_index(shape)
        wave_x = (lax.broadcasted_iota(jnp.int32, shape, 0) - MODES // 2).astype(F32) / (CELLS // 4)
        wave_y = (lane // 32 + LINES_Y * pair - MODES // 2).astype(F32) / (CELLS // 4)
        wave_z = ((lane & 7) + 8 * gy).astype(F32) / (CELLS // 4)
        factor[0] = -DIFFUSE * (wave_x * wave_x + wave_y * wave_y + wave_z * wave_z) * NORM
        factor[1] = -(0.3 * wave_x + 0.2 * wave_y + 0.25 * wave_z) * NORM
        edge = (wave_z == 0.0) & ((wave_x == -1.0) | (wave_y == -1.0))
        factor[2] = jnp.where(edge, 0.5 / NORM, 1.0 / NORM)

    def z_forward(first, second):
        lines = times_table(jnp.concatenate([first, second], axis=0), tz)
        mats = [
            lines[(field * SLAB + i) * ROWS_Y : (field * SLAB + i + 1) * ROWS_Y]
            for i in range(SLAB)
            for field in range(2)
        ]
        for part, mat in enumerate(swap_groups(mats)):
            y_send[part] = mat

    def z_back(mats):
        lines = swap_groups(mats)
        stacked = jnp.concatenate([lines[2 * i + f] for f in range(2) for i in range(SLAB)], axis=0)
        values = times_table(stacked, bz)
        half = SLAB * ROWS_Y
        return values[:half], values[half:]

    def y_forward():
        both = table_times(ty, y_recv[...].reshape(CELLS, LANES))
        lines = both[:MODES] - turn(both[MODES:])
        x_send.reshape(MODES, LANES)[...] = lines

    def x_middle(x_recv, carried):
        rows = x_recv.reshape(CELLS, LANES)
        mats = [rows[pl.ds(ky, PLANE, stride=LINES_Y), :] for ky in range(LINES_Y)]
        lines = jnp.concatenate(swap_groups(mats), axis=0)
        both = table_times(tx, lines)
        cosine, sine = both[:MODES], both[MODES:]
        real, imag = factor[0], factor[1]
        first = (lane_index(cosine.shape) & 16) == 0
        spectrum, turned = cosine - turn(sine), turn(cosine) + sine
        if carried:
            spectrum, turned = spectrum + carry[0], turned + carry[1]
        rate = real * spectrum + imag * turned
        rate_turned = real * turned - imag * spectrum
        spectrum = factor[2] * roll(rate, 16) + spectrum
        turned = factor[2] * roll(rate_turned, 16) + turned
        rate = jnp.where(first, rate, real * spectrum + imag * turned)
        rate_turned = jnp.where(first, rate_turned, real * turned - imag * spectrum)
        if not carried:
            carry[0] = rate
            carry[1] = rate_turned
        lines = table_times(bx, jnp.concatenate([rate, rate_turned], axis=0))
        target = b_send.reshape(CELLS, LANES)
        mats = [lines[i * PLANE : (i + 1) * PLANE] for i in range(SLAB)]
        for ky, mat in enumerate(swap_groups(mats)):
            target[pl.ds(ky, PLANE, stride=LINES_Y), :] = mat

    def prepare_carry():
        first = (lane_index((MODES, LANES)) & 16) == 0
        for i in range(2):
            carry[i] = jnp.where(first, factor[2] * roll(carry[i], -16), 0.0)

    def y_back():
        lines = b_recv.reshape(MODES, LANES)[...]
        cells = table_times(by, jnp.concatenate([lines, turn(lines)], axis=0))
        u_send[...] = cells.reshape(PARTS_Y, ROWS_Y, LANES)

    for i in range(3):
        loads[i].wait()
    start = v[...].reshape(SLAB * ROWS_Y, CELLS)
    react = r[...].reshape(SLAB * ROWS_Y, CELLS)
    z_forward(start, react * start)
    for i in range(3, 8):
        loads[i].wait()
    pl.semaphore_wait(barrier, heard)
    for dy in (3, 0):
        for dz in (4, RING_Z - 4):
            pl.semaphore_signal(
                ready, inc=1, device_id=plane_id(*place(dy, dz)), device_id_type=MESH
            )

    others_y = pl.ds(0, PARTS_Y - 1)
    others_x = pl.ds(0, PLANE - 1)
    others_b = pl.ds(0, PAIRS - 1)
    y_exchange(y_send, y_recv, Y_OUT)
    prepare_factor()
    received(y_recv.at[others_y], Y_OUT)
    y_forward()
    pl.semaphore_wait(ready, 4)
    x_exchange(x_recv1, X_OUT)
    received(x_recv1.at[others_x], X_OUT)
    x_middle(x_recv1, False)
    x_return(X_BACK, 0)
    prepare_carry()
    received(b_recv.at[others_b], X_BACK)
    y_back()
    sent(y_send.at[others_y], Y_OUT)
    y_exchange(u_send, u_recv, Y_BACK)
    received(u_recv.at[others_y], Y_BACK)
    smooth, smooth_rate = z_back([u_recv[part] for part in range(PARTS_Y)])
    rate1 = smooth + react * start
    rate2 = smooth_rate + react * rate1
    z_forward(react * rate1, react * rate2)

    sent(x_recv1.at[others_x], X_OUT)
    sent(b_send.at[others_b], X_BACK)
    y_exchange(y_send, y_recv, Y_OUT2)
    known = start + rate1
    piece_send[0] = known.reshape(SLAB, ROWS_Y, CELLS)
    known = known + 0.5 * rate2
    piece_send[1] = known.reshape(SLAB, ROWS_Y, CELLS)
    known = known + 0.25 * (react * rate2)
    piece_send[2] = known.reshape(SLAB, ROWS_Y, CELLS)
    known = known + 0.125 * (react * (react * rate2))
    piece_send[3] = known.reshape(SLAB, ROWS_Y, CELLS)

    def send_pieces(point):
        for level in range(LEVELS):
            cuts = (0, *CUTS[level // 2])

            @pl.when(lvl != level)
            def _(level=level, cuts=cuts):
                for at in range(cuts[point], cuts[point + 1]):
                    half = pl.ds(at % 2 * (ROWS_Y // 2), ROWS_Y // 2)
                    source = piece_send.at[level, at // 2, half]
                    target = piece.at[lvl * SLAB + at // 2, half]
                    remote(source, target, BULK, {"lvl": level}).start()

    send_pieces(0)
    piece[own] = piece_send[lvl]

    received(y_recv.at[others_y], Y_OUT2)
    y_forward()
    x_exchange(x_recv2, X_OUT2)
    send_pieces(1)
    received(x_recv2.at[others_x], X_OUT2)
    x_middle(x_recv2, True)
    x_return(X_BACK2, 1)
    send_pieces(2)
    received(b_recv.at[others_b], X_BACK2)
    sent(u_send.at[others_y], Y_BACK)
    y_back()

    before = lax.rem(at_z + RING_Z - 1, RING_Z)
    slab, block = lax.rem(before, 4), row_y * 4 + lax.div(before, 4)

    def last(level, k):
        other = lax.rem(gy + k, PARTS_Y)
        remote(
            u_send.at[other],
            f_recv.at[slab, gy],
            FINAL + slab,
            {"lvl": level, "gx": block, "gy": other},
            FINAL + level,
        ).start()

    for k in (4, 3, 5, 2, 6, 1, 7):
        for level in (3, 2):
            last(level, k)
    for level in (3, 2):
        @pl.when(lvl != level)
        def _(level=level):
            last(level, 0)

        @pl.when(lvl == level)
        def _():
            f_recv[slab, gy] = u_send[gy]

    send_pieces(3)
    loads[8].wait()
    received(piece.at[pl.ds(0, ROWS_X - SLAB)], BULK)

    @pl.when(lvl >= 2)
    def _():
        last_weight = jnp.where(lvl == 3, 0.125, 0.0)
        for step in (0, 3, 1, 2):
            t = lax.rem(lvl - 1 + step, LEVELS)
            if step == 0:
                received(f_recv.at[t, others_y], FINAL + t)
            else:
                received(f_recv.at[t], FINAL + t)
            first, second = z_back([f_recv[t, part] for part in range(PARTS_Y)])
            at = pl.ds(t * SLAB, SLAB)
            first = first.reshape(SLAB, ROWS_Y, CELLS)
            second = second.reshape(SLAB, ROWS_Y, CELLS)
            piece[at] = piece[at] + (0.25 + last_weight * r_all[at]) * first + last_weight * second


    sent(y_send.at[others_y], Y_OUT2)
    sent(x_recv2.at[others_x], X_OUT2)
    sent(b_send.at[others_b], X_BACK2)
    sent(piece_send.at[pl.ds(0, 3)], BULK)
    for level in (3, 2):
        @pl.when(lvl != level)
        def _(level=level):
            sent(u_send, FINAL + level)

        @pl.when(lvl == level)
        def _(level=level):
            sent(u_send.at[others_y], FINAL + level)


def solution(mesh):
    constants = tables()

    def shards(initial, reaction):
        rows = (SLAB, ROWS_Y, CELLS)
        block = (ROWS_X, ROWS_Y, CELLS)
        lines = (PARTS_Y, ROWS_Y, LANES)
        chunks = (PLANE, LINES_Y, LANES)
        half_chunks = (PAIRS, LINES_Y, LANES)
        vmem = pltpu.VMEM
        result = pl.pallas_call(
            kernel,
            out_shape=pltpu.VMEM(block, F32),
            in_specs=[pl.BlockSpec(memory_space=pl.ANY)] * 8,
            out_specs=pl.BlockSpec(memory_space=pltpu.VMEM),
            scratch_shapes=[
                vmem(rows, F32),
                vmem(rows, F32),
                vmem(block, F32),
                *[vmem(t.shape, BF16) for t in constants],
                vmem((3, MODES, LANES), F32),
                vmem((2, MODES, LANES), F32),
                vmem(lines, F32),
                vmem(lines, F32),
                vmem(half_chunks, F32),
                vmem(chunks, F32),
                vmem(chunks, F32),
                vmem(chunks, F32),
                vmem(half_chunks, F32),
                vmem(lines, F32),
                vmem(lines, F32),
                vmem((LEVELS, *lines), F32),
                vmem((LEVELS, *rows), F32),
                pltpu.SemaphoreType.DMA((9,)),
                pltpu.SemaphoreType.DMA((PHASES,)),
                pltpu.SemaphoreType.DMA((PHASES,)),
                pltpu.SemaphoreType.REGULAR,
            ],
            compiler_params=pltpu.CompilerParams(collective_id=0, has_side_effects=True),
        )(initial, reaction, *[jnp.asarray(t) for t in constants])
        return result[None]

    in_specs = (P("gx", "gy", None), P("gx", "gy", None))
    out_specs = P("lvl", "gx", "gy", None)
    return jax.shard_map(shards, mesh=mesh, in_specs=in_specs, out_specs=out_specs, check_vma=False)
```

```python
import functools
import math

import jax
import jax.numpy as jnp
import numpy as np
from jax import lax
from jax.experimental import pallas as pl
from jax.experimental.pallas import tpu as pltpu
from jax.sharding import PartitionSpec as P

CELLS = 256
MODES = 128
DEPTH_MODES = 64
LEVELS = 4
PARTS_X = 16
PARTS_Y = 8
PLANE = LEVELS * PARTS_X
SLAB = CELLS // PLANE
PAIRS = PLANE // 2
LINES_Y = MODES // PAIRS
ROWS_Y = CELLS // PARTS_Y
ROWS_X = CELLS // PARTS_X
RING_Z = 16
RING_Y = 4
DIFFUSE = 0.3
NORM = 1.0 / CELLS**3
LANES = 128
MESH = pl.DeviceIdType.MESH
F32 = jnp.float32
BF16 = jnp.bfloat16

Y_OUT, X_OUT, X_BACK, Y_BACK, Y_OUT2, X_OUT2, X_BACK2, BULK, FINAL = range(9)
PHASES = FINAL + LEVELS
CUTS = ((1, 2, 6, 8), (2, 4, 8, 8))


def halves(table):
    high = table.astype(BF16)
    low = (table - high.astype(np.float64)).astype(BF16)
    return np.concatenate([high, low], axis=0)


def tables():
    points = np.arange(CELLS)
    step = 2.0 * math.pi / CELLS

    def phase(wave):
        angle = (points[:, None] * wave[None, :] % CELLS) * step
        return np.cos(angle), np.sin(angle)

    wave_z = np.arange(DEPTH_MODES)
    cos_z, sin_z = phase(wave_z)
    per_part = DEPTH_MODES // PARTS_Y

    def parts(real, imag):
        stacked = np.stack([real, imag], axis=1)
        stacked = stacked.reshape(CELLS, 2, PARTS_Y, per_part)
        return stacked.transpose(0, 2, 1, 3).reshape(CELLS, LANES)

    forward_z = parts(cos_z, -sin_z)
    weight = np.where(wave_z == 0, 1.0, 2.0)
    back_z = parts(cos_z * weight, -sin_z * weight).T

    wave = np.arange(MODES) - MODES // 2
    cosine, sine = phase(wave)
    forward_y = np.concatenate([cosine.T, sine.T], axis=0)
    back_y = np.concatenate([cosine, sine], axis=1)
    order = (np.arange(PLANE)[None, :] * SLAB + np.arange(SLAB)[:, None]).reshape(-1)
    forward_x = forward_y[:, order]
    back_x = back_y[order, :]
    return [halves(t) for t in (forward_z, forward_y, forward_x, back_x, back_y, back_z)]


def split(x):
    high = x.astype(BF16)
    return high, (x - high.astype(F32)).astype(BF16)


def dot(a, b):
    return jnp.dot(a, b, preferred_element_type=F32)


def table_times(table, data):
    rows = table.shape[0] // 2
    high, low = split(data)
    first = dot(table[...], high)
    return first[:rows] + first[rows:] + dot(table[:rows, :], low)


def times_table(data, table):
    depth = table.shape[0] // 2
    rows = data.shape[0]
    high, low = split(data)
    first = dot(jnp.concatenate([high, low], axis=0), table[:depth, :])
    return first[:rows] + first[rows:] + dot(high, table[depth:, :])


def lane_index(shape):
    return lax.broadcasted_iota(jnp.int32, shape, 1)


def roll(x, shift):
    return x if shift % LANES == 0 else pltpu.roll(x, shift % LANES, 1)


def turn(x):
    real = (lane_index(x.shape) & 8) == 0
    return jnp.where(real, -roll(x, -8), roll(x, 8))


def swap_groups(mats):
    mats = list(mats)
    count = len(mats)
    width = LANES // count
    group = lane_index(mats[0].shape) // width
    bit = 1
    while bit < count:
        keep = (group & bit) == 0
        for low in range(count):
            if low & bit:
                continue
            high = low | bit
            a, b = mats[low], mats[high]
            mats[low] = jnp.where(keep, a, roll(b, width * bit))
            mats[high] = jnp.where(keep, roll(a, -width * bit), b)
        bit *= 2
    return mats


def hops(dy, dz):
    return min(dy, RING_Y - dy) + min(dz, RING_Z - dz)


def offsets():
    every = [(dy, dz) for dz in range(RING_Z) for dy in range(RING_Y) if (dy, dz) != (0, 0)]
    every.sort(key=lambda o: -hops(*o))
    near = []
    for dy, dz in every:
        opposite = ((dy + 2) % RING_Y, (dz + 8) % RING_Z)
        if opposite not in near and hops(dy, dz) <= hops(*opposite):
            near.append((dy, dz))
    return every, near


def kernel(
    v_hbm, r_hbm, tz_hbm, ty_hbm, tx_hbm, bx_hbm, by_hbm, bz_hbm, piece,
    v, r, r_all, tz, ty, tx, bx, by, bz,
    factor, carry, y_send, y_recv, x_send, x_recv1, x_recv2, b_send, b_recv, u_send, u_recv, f_recv,
    piece_send, load_sem, send_sem, recv_sem, ready,
):
    lvl, gx, gy = lax.axis_index("lvl"), lax.axis_index("gx"), lax.axis_index("gy")
    row_y, high_z = lax.div(gx, 4), lax.rem(gx, 4)
    at_z = high_z * 4 + lvl
    me = row_y * RING_Z + at_z

    pair = lax.rem(row_y, 2) * RING_Z + lax.rem(at_z + 8 * lax.div(row_y, 2), RING_Z)

    def place(dy, dz):
        return lax.rem(row_y + dy, RING_Y), lax.rem(at_z + dz, RING_Z)

    def plane_id(y2, z2):
        return {"gx": y2 * 4 + lax.div(z2, 4), "lvl": lax.rem(z2, 4)}

    every, near = offsets()

    own = pl.ds(lvl * SLAB, SLAB)
    loads = [
        pltpu.make_async_copy(source, target, load_sem.at[i])
        for i, (source, target) in enumerate(
            [
                (v_hbm.at[own], v),
                (r_hbm.at[own], r),
                (tz_hbm, tz),
                (ty_hbm, ty),
                (tx_hbm, tx),
                (bx_hbm, bx),
                (by_hbm, by),
                (bz_hbm, bz),
                (r_hbm, r_all),
            ]
        )
    ]
    for load in loads[:3]:
        load.start()

    barrier = pltpu.get_barrier_semaphore()
    heard = 0
    for dy, dz in every:
        if min(dz, RING_Z - dz) <= 4 and dy != 2:
            pl.semaphore_signal(
                barrier, inc=1, device_id=plane_id(*place(dy, dz)), device_id_type=MESH
            )
            heard += 1
    for k in (4, 3, 5, 2, 6, 1, 7):
        pl.semaphore_signal(
            barrier, inc=1, device_id={"gy": lax.rem(gy + k, PARTS_Y)}, device_id_type=MESH
        )
        heard += 1
    for load in loads[3:]:
        load.start()

    def remote(source, target, phase, device_id, send_phase=None):
        return pltpu.make_async_remote_copy(
            src_ref=source,
            dst_ref=target,
            send_sem=send_sem.at[phase if send_phase is None else send_phase],
            recv_sem=recv_sem.at[phase],
            device_id=device_id,
            device_id_type=MESH,
        )

    def received(ref, phase):
        remote(ref, ref, phase, {"gy": gy}).wait_recv()

    def sent(ref, phase):
        remote(ref, ref, phase, {"gy": gy}).wait_send()

    def y_exchange(source, target, phase):
        for k in (4, 3, 5, 2, 6, 1, 7):
            other = lax.rem(gy + k, PARTS_Y)
            remote(source.at[other], target.at[gy], phase, {"gy": other}).start()
        target[gy] = source[gy]

    def x_exchange(x_recv, phase):
        def send(y2, z2):
            chunk = lax.rem(y2, 2) * RING_Z + lax.rem(z2 + 8 * lax.div(y2, 2), RING_Z)
            remote(x_send.at[chunk], x_recv.at[me], phase, plane_id(y2, z2)).start()

        for dy, dz in every:
            send(*place(dy, dz))
        x_recv[me] = x_send[pair]

    def x_return(phase, shift):
        def chunk_of(y2, z2):
            return y2 * RING_Z + lax.rem(z2 + RING_Z - shift, RING_Z)

        for dy, dz in near:
            y2, z2 = place(dy, dz)
            remote(b_send.at[chunk_of(y2, z2)], b_recv.at[pair], phase, plane_id(y2, z2)).start()
        b_recv[pair] = b_send[chunk_of(row_y, at_z)]

    def prepare_factor():
        shape = (MODES, LANES)
        lane = lane_index(shape)
        wave_x = (lax.broadcasted_iota(jnp.int32, shape, 0) - MODES // 2).astype(F32) / (CELLS // 4)
        wave_y = (lane // 32 + LINES_Y * pair - MODES // 2).astype(F32) / (CELLS // 4)
        wave_z = ((lane & 7) + 8 * gy).astype(F32) / (CELLS // 4)
        factor[0] = -DIFFUSE * (wave_x * wave_x + wave_y * wave_y + wave_z * wave_z) * NORM
        factor[1] = -(0.3 * wave_x + 0.2 * wave_y + 0.25 * wave_z) * NORM
        edge = (wave_z == 0.0) & ((wave_x == -1.0) | (wave_y == -1.0))
        factor[2] = jnp.where(edge, 0.5 / NORM, 1.0 / NORM)

    def z_forward(first, second):
        lines = times_table(jnp.concatenate([first, second], axis=0), tz)
        mats = [
            lines[(field * SLAB + i) * ROWS_Y : (field * SLAB + i + 1) * ROWS_Y]
            for i in range(SLAB)
            for field in range(2)
        ]
        for part, mat in enumerate(swap_groups(mats)):
            y_send[part] = mat

    def z_back(mats):
        lines = swap_groups(mats)
        stacked = jnp.concatenate([lines[2 * i + f] for f in range(2) for i in range(SLAB)], axis=0)
        values = times_table(stacked, bz)
        half = SLAB * ROWS_Y
        return values[:half], values[half:]

    def y_forward():
        both = table_times(ty, y_recv[...].reshape(CELLS, LANES))
        lines = both[:MODES] - turn(both[MODES:])
        x_send.reshape(MODES, LANES)[...] = lines

    def x_middle(x_recv, carried):
        rows = x_recv.reshape(CELLS, LANES)
        mats = [rows[pl.ds(ky, PLANE, stride=LINES_Y), :] for ky in range(LINES_Y)]
        lines = jnp.concatenate(swap_groups(mats), axis=0)
        both = table_times(tx, lines)
        cosine, sine = both[:MODES], both[MODES:]
        real, imag = factor[0], factor[1]
        first = (lane_index(cosine.shape) & 16) == 0
        spectrum, turned = cosine - turn(sine), turn(cosine) + sine
        if carried:
            spectrum, turned = spectrum + carry[0], turned + carry[1]
        rate = real * spectrum + imag * turned
        rate_turned = real * turned - imag * spectrum
        spectrum = factor[2] * roll(rate, 16) + spectrum
        turned = factor[2] * roll(rate_turned, 16) + turned
        rate = jnp.where(first, rate, real * spectrum + imag * turned)
        rate_turned = jnp.where(first, rate_turned, real * turned - imag * spectrum)
        if not carried:
            carry[0] = rate
            carry[1] = rate_turned
        lines = table_times(bx, jnp.concatenate([rate, rate_turned], axis=0))
        target = b_send.reshape(CELLS, LANES)
        mats = [lines[i * PLANE : (i + 1) * PLANE] for i in range(SLAB)]
        for ky, mat in enumerate(swap_groups(mats)):
            target[pl.ds(ky, PLANE, stride=LINES_Y), :] = mat

    def prepare_carry():
        first = (lane_index((MODES, LANES)) & 16) == 0
        for i in range(2):
            carry[i] = jnp.where(first, factor[2] * roll(carry[i], -16), 0.0)

    def y_back():
        lines = b_recv.reshape(MODES, LANES)[...]
        cells = table_times(by, jnp.concatenate([lines, turn(lines)], axis=0))
        u_send[...] = cells.reshape(PARTS_Y, ROWS_Y, LANES)

    for i in range(3):
        loads[i].wait()
    start = v[...].reshape(SLAB * ROWS_Y, CELLS)
    react = r[...].reshape(SLAB * ROWS_Y, CELLS)
    z_forward(start, react * start)
    for i in range(3, 8):
        loads[i].wait()
    pl.semaphore_wait(barrier, heard)
    for dy in (3, 0):
        for dz in (4, RING_Z - 4):
            pl.semaphore_signal(
                ready, inc=1, device_id=plane_id(*place(dy, dz)), device_id_type=MESH
            )

    others_y = pl.ds(0, PARTS_Y - 1)
    others_x = pl.ds(0, PLANE - 1)
    others_b = pl.ds(0, PAIRS - 1)
    y_exchange(y_send, y_recv, Y_OUT)
    prepare_factor()
    received(y_recv.at[others_y], Y_OUT)
    y_forward()
    pl.semaphore_wait(ready, 4)
    x_exchange(x_recv1, X_OUT)
    received(x_recv1.at[others_x], X_OUT)
    x_middle(x_recv1, False)
    x_return(X_BACK, 0)
    prepare_carry()
    received(b_recv.at[others_b], X_BACK)
    y_back()
    sent(y_send.at[others_y], Y_OUT)
    y_exchange(u_send, u_recv, Y_BACK)
    received(u_recv.at[others_y], Y_BACK)
    smooth, smooth_rate = z_back([u_recv[part] for part in range(PARTS_Y)])
    rate1 = smooth + react * start
    rate2 = smooth_rate + react * rate1
    z_forward(react * rate1, react * rate2)

    sent(x_recv1.at[others_x], X_OUT)
    sent(b_send.at[others_b], X_BACK)
    y_exchange(y_send, y_recv, Y_OUT2)
    known = start + rate1
    piece_send[0] = known.reshape(SLAB, ROWS_Y, CELLS)
    known = known + 0.5 * rate2
    piece_send[1] = known.reshape(SLAB, ROWS_Y, CELLS)
    known = known + 0.25 * (react * rate2)
    piece_send[2] = known.reshape(SLAB, ROWS_Y, CELLS)
    known = known + 0.125 * (react * (react * rate2))
    piece_send[3] = known.reshape(SLAB, ROWS_Y, CELLS)

    def send_pieces(point):
        for level in range(LEVELS):
            cuts = (0, *CUTS[level // 2])

            @pl.when(lvl != level)
            def _(level=level, cuts=cuts):
                for at in range(cuts[point], cuts[point + 1]):
                    half = pl.ds(at % 2 * (ROWS_Y // 2), ROWS_Y // 2)
                    source = piece_send.at[level, at // 2, half]
                    target = piece.at[lvl * SLAB + at // 2, half]
                    remote(source, target, BULK, {"lvl": level}).start()

    send_pieces(0)
    piece[own] = piece_send[lvl]

    received(y_recv.at[others_y], Y_OUT2)
    y_forward()
    x_exchange(x_recv2, X_OUT2)
    send_pieces(1)
    received(x_recv2.at[others_x], X_OUT2)
    x_middle(x_recv2, True)
    x_return(X_BACK2, 1)
    send_pieces(2)
    received(b_recv.at[others_b], X_BACK2)
    sent(u_send.at[others_y], Y_BACK)
    y_back()

    before = lax.rem(at_z + RING_Z - 1, RING_Z)
    slab, block = lax.rem(before, 4), row_y * 4 + lax.div(before, 4)

    def last(level, k):
        other = lax.rem(gy + k, PARTS_Y)
        remote(
            u_send.at[other],
            f_recv.at[slab, gy],
            FINAL + slab,
            {"lvl": level, "gx": block, "gy": other},
            FINAL + level,
        ).start()

    for k in (4, 3, 5, 2, 6, 1, 7):
        for level in (3, 2):
            last(level, k)
    for level in (3, 2):
        @pl.when(lvl != level)
        def _(level=level):
            last(level, 0)

        @pl.when(lvl == level)
        def _():
            f_recv[slab, gy] = u_send[gy]

    send_pieces(3)
    loads[8].wait()
    received(piece.at[pl.ds(0, ROWS_X - SLAB)], BULK)

    @pl.when(lvl >= 2)
    def _():
        last_weight = jnp.where(lvl == 3, 0.125, 0.0)
        def add(steps):
            slabs = [lax.rem(lvl - 1 + step, LEVELS) for step in steps]
            for t, step in zip(slabs, steps):
                received(f_recv.at[t] if step else f_recv.at[t, others_y], FINAL + t)
            parts = [z_back([f_recv[t, part] for part in range(PARTS_Y)]) for t in slabs]
            for t, (first, second) in zip(slabs, parts):
                at = pl.ds(t * SLAB, SLAB)
                first = first.reshape(SLAB, ROWS_Y, CELLS)
                second = second.reshape(SLAB, ROWS_Y, CELLS)
                scale = 0.25 + last_weight * r_all[at]
                piece[at] = piece[at] + scale * first + last_weight * second

        add((0,))
        add((3, 1, 2))

    sent(y_send.at[others_y], Y_OUT2)
    sent(x_recv2.at[others_x], X_OUT2)
    sent(b_send.at[others_b], X_BACK2)
    sent(piece_send.at[pl.ds(0, 3)], BULK)
    for level in (3, 2):
        @pl.when(lvl != level)
        def _(level=level):
            sent(u_send, FINAL + level)

        @pl.when(lvl == level)
        def _(level=level):
            sent(u_send.at[others_y], FINAL + level)


def solution(mesh):
    constants = tables()

    def shards(initial, reaction):
        rows = (SLAB, ROWS_Y, CELLS)
        block = (ROWS_X, ROWS_Y, CELLS)
        lines = (PARTS_Y, ROWS_Y, LANES)
        chunks = (PLANE, LINES_Y, LANES)
        half_chunks = (PAIRS, LINES_Y, LANES)
        vmem = pltpu.VMEM
        result = pl.pallas_call(
            kernel,
            out_shape=pltpu.VMEM(block, F32),
            in_specs=[pl.BlockSpec(memory_space=pl.ANY)] * 8,
            out_specs=pl.BlockSpec(memory_space=pltpu.VMEM),
            scratch_shapes=[
                vmem(rows, F32),
                vmem(rows, F32),
                vmem(block, F32),
                *[vmem(t.shape, BF16) for t in constants],
                vmem((3, MODES, LANES), F32),
                vmem((2, MODES, LANES), F32),
                vmem(lines, F32),
                vmem(lines, F32),
                vmem(half_chunks, F32),
                vmem(chunks, F32),
                vmem(chunks, F32),
                vmem(chunks, F32),
                vmem(half_chunks, F32),
                vmem(lines, F32),
                vmem(lines, F32),
                vmem((LEVELS, *lines), F32),
                vmem((LEVELS, *rows), F32),
                pltpu.SemaphoreType.DMA((9,)),
                pltpu.SemaphoreType.DMA((PHASES,)),
                pltpu.SemaphoreType.DMA((PHASES,)),
                pltpu.SemaphoreType.REGULAR,
            ],
            compiler_params=pltpu.CompilerParams(collective_id=0, has_side_effects=True),
        )(initial, reaction, *[jnp.asarray(t) for t in constants])
        return result[None]

    in_specs = (P("gx", "gy", None), P("gx", "gy", None))
    out_specs = P("lvl", "gx", "gy", None)
    return jax.shard_map(shards, mesh=mesh, in_specs=in_specs, out_specs=out_specs, check_vma=False)
```

```python
import functools
import math

import jax
import jax.numpy as jnp
import numpy as np
from jax import lax
from jax.experimental import pallas as pl
from jax.experimental.pallas import tpu as pltpu
from jax.sharding import PartitionSpec as P

CELLS = 256
MODES = 128
DEPTH_MODES = 64
LEVELS = 4
PARTS_X = 16
PARTS_Y = 8
PLANE = LEVELS * PARTS_X
SLAB = CELLS // PLANE
PAIRS = PLANE // 2
LINES_Y = MODES // PAIRS
ROWS_Y = CELLS // PARTS_Y
ROWS_X = CELLS // PARTS_X
RING_Z = 16
RING_Y = 4
DIFFUSE = 0.3
NORM = 1.0 / CELLS**3
LANES = 128
MESH = pl.DeviceIdType.MESH
F32 = jnp.float32
BF16 = jnp.bfloat16

Y_OUT, X_OUT, X_BACK, Y_BACK, Y_OUT2, X_OUT2, X_BACK2, BULK, FINAL = range(9)
PHASES = FINAL + LEVELS
CUTS = ((1, 3, 7, 8), (2, 4, 8, 8))


def halves(table):
    high = table.astype(BF16)
    low = (table - high.astype(np.float64)).astype(BF16)
    return np.concatenate([high, low], axis=0)


def tables():
    points = np.arange(CELLS)
    step = 2.0 * math.pi / CELLS

    def phase(wave):
        angle = (points[:, None] * wave[None, :] % CELLS) * step
        return np.cos(angle), np.sin(angle)

    wave_z = np.arange(DEPTH_MODES)
    cos_z, sin_z = phase(wave_z)
    per_part = DEPTH_MODES // PARTS_Y

    def parts(real, imag):
        stacked = np.stack([real, imag], axis=1)
        stacked = stacked.reshape(CELLS, 2, PARTS_Y, per_part)
        return stacked.transpose(0, 2, 1, 3).reshape(CELLS, LANES)

    forward_z = parts(cos_z, -sin_z)
    weight = np.where(wave_z == 0, 1.0, 2.0)
    back_z = parts(cos_z * weight, -sin_z * weight).T

    wave = np.arange(MODES) - MODES // 2
    cosine, sine = phase(wave)
    forward_y = np.concatenate([cosine.T, sine.T], axis=0)
    back_y = np.concatenate([cosine, sine], axis=1)
    order = (np.arange(PLANE)[None, :] * SLAB + np.arange(SLAB)[:, None]).reshape(-1)
    forward_x = forward_y[:, order]
    back_x = back_y[order, :]
    return [halves(t) for t in (forward_z, forward_y, forward_x, back_x, back_y, back_z)]


def split(x):
    high = x.astype(BF16)
    return high, (x - high.astype(F32)).astype(BF16)


def dot(a, b):
    return jnp.dot(a, b, preferred_element_type=F32)


def table_times(table, data):
    rows = table.shape[0] // 2
    high, low = split(data)
    first = dot(table[...], high)
    return first[:rows] + first[rows:] + dot(table[:rows, :], low)


def times_table(data, table):
    depth = table.shape[0] // 2
    rows = data.shape[0]
    high, low = split(data)
    first = dot(jnp.concatenate([high, low], axis=0), table[:depth, :])
    return first[:rows] + first[rows:] + dot(high, table[depth:, :])


def lane_index(shape):
    return lax.broadcasted_iota(jnp.int32, shape, 1)


def roll(x, shift):
    return x if shift % LANES == 0 else pltpu.roll(x, shift % LANES, 1)


def turn(x):
    real = (lane_index(x.shape) & 8) == 0
    return jnp.where(real, -roll(x, -8), roll(x, 8))


def swap_groups(mats):
    mats = list(mats)
    count = len(mats)
    width = LANES // count
    group = lane_index(mats[0].shape) // width
    bit = 1
    while bit < count:
        keep = (group & bit) == 0
        for low in range(count):
            if low & bit:
                continue
            high = low | bit
            a, b = mats[low], mats[high]
            mats[low] = jnp.where(keep, a, roll(b, width * bit))
            mats[high] = jnp.where(keep, roll(a, -width * bit), b)
        bit *= 2
    return mats


def hops(dy, dz):
    return min(dy, RING_Y - dy) + min(dz, RING_Z - dz)


def offsets():
    every = [(dy, dz) for dz in range(RING_Z) for dy in range(RING_Y) if (dy, dz) != (0, 0)]
    every.sort(key=lambda o: -hops(*o))
    near = []
    for dy, dz in every:
        opposite = ((dy + 2) % RING_Y, (dz + 8) % RING_Z)
        if opposite not in near and hops(dy, dz) <= hops(*opposite):
            near.append((dy, dz))
    return every, near


def kernel(
    v_hbm, r_hbm, tz_hbm, ty_hbm, tx_hbm, bx_hbm, by_hbm, bz_hbm, piece,
    v, r, r_all, tz, ty, tx, bx, by, bz,
    factor, carry, y_send, y_recv, x_send, x_recv1, x_recv2, b_send, b_recv, u_send, u_recv, f_recv,
    piece_send, load_sem, send_sem, recv_sem, ready,
):
    lvl, gx, gy = lax.axis_index("lvl"), lax.axis_index("gx"), lax.axis_index("gy")
    row_y, high_z = lax.div(gx, 4), lax.rem(gx, 4)
    at_z = high_z * 4 + lvl
    me = row_y * RING_Z + at_z

    pair = lax.rem(row_y, 2) * RING_Z + lax.rem(at_z + 8 * lax.div(row_y, 2), RING_Z)

    def place(dy, dz):
        return lax.rem(row_y + dy, RING_Y), lax.rem(at_z + dz, RING_Z)

    def plane_id(y2, z2):
        return {"gx": y2 * 4 + lax.div(z2, 4), "lvl": lax.rem(z2, 4)}

    every, near = offsets()

    own = pl.ds(lvl * SLAB, SLAB)
    loads = [
        pltpu.make_async_copy(source, target, load_sem.at[i])
        for i, (source, target) in enumerate(
            [
                (v_hbm.at[own], v),
                (r_hbm.at[own], r),
                (tz_hbm, tz),
                (ty_hbm, ty),
                (tx_hbm, tx),
                (bx_hbm, bx),
                (by_hbm, by),
                (bz_hbm, bz),
                (r_hbm, r_all),
            ]
        )
    ]
    for load in loads[:3]:
        load.start()

    barrier = pltpu.get_barrier_semaphore()
    heard = 0
    for dy, dz in every:
        if min(dz, RING_Z - dz) <= 4 and dy != 2:
            pl.semaphore_signal(
                barrier, inc=1, device_id=plane_id(*place(dy, dz)), device_id_type=MESH
            )
            heard += 1
    for k in (4, 3, 5, 2, 6, 1, 7):
        pl.semaphore_signal(
            barrier, inc=1, device_id={"gy": lax.rem(gy + k, PARTS_Y)}, device_id_type=MESH
        )
        heard += 1
    for load in loads[3:]:
        load.start()

    def remote(source, target, phase, device_id, send_phase=None):
        return pltpu.make_async_remote_copy(
            src_ref=source,
            dst_ref=target,
            send_sem=send_sem.at[phase if send_phase is None else send_phase],
            recv_sem=recv_sem.at[phase],
            device_id=device_id,
            device_id_type=MESH,
        )

    def received(ref, phase):
        remote(ref, ref, phase, {"gy": gy}).wait_recv()

    def sent(ref, phase):
        remote(ref, ref, phase, {"gy": gy}).wait_send()

    def y_exchange(source, target, phase):
        for k in (4, 3, 5, 2, 6, 1, 7):
            other = lax.rem(gy + k, PARTS_Y)
            remote(source.at[other], target.at[gy], phase, {"gy": other}).start()
        target[gy] = source[gy]

    def x_exchange(x_recv, phase):
        def send(y2, z2):
            chunk = lax.rem(y2, 2) * RING_Z + lax.rem(z2 + 8 * lax.div(y2, 2), RING_Z)
            remote(x_send.at[chunk], x_recv.at[me], phase, plane_id(y2, z2)).start()

        for dy, dz in every:
            send(*place(dy, dz))
        x_recv[me] = x_send[pair]

    def x_return(phase, shift):
        def chunk_of(y2, z2):
            return y2 * RING_Z + lax.rem(z2 + RING_Z - shift, RING_Z)

        for dy, dz in near:
            y2, z2 = place(dy, dz)
            remote(b_send.at[chunk_of(y2, z2)], b_recv.at[pair], phase, plane_id(y2, z2)).start()
        b_recv[pair] = b_send[chunk_of(row_y, at_z)]

    def prepare_factor():
        shape = (MODES, LANES)
        lane = lane_index(shape)
        wave_x = (lax.broadcasted_iota(jnp.int32, shape, 0) - MODES // 2).astype(F32) / (CELLS // 4)
        wave_y = (lane // 32 + LINES_Y * pair - MODES // 2).astype(F32) / (CELLS // 4)
        wave_z = ((lane & 7) + 8 * gy).astype(F32) / (CELLS // 4)
        factor[0] = -DIFFUSE * (wave_x * wave_x + wave_y * wave_y + wave_z * wave_z) * NORM
        factor[1] = -(0.3 * wave_x + 0.2 * wave_y + 0.25 * wave_z) * NORM
        edge = (wave_z == 0.0) & ((wave_x == -1.0) | (wave_y == -1.0))
        factor[2] = jnp.where(edge, 0.5 / NORM, 1.0 / NORM)

    def z_forward(first, second):
        lines = times_table(jnp.concatenate([first, second], axis=0), tz)
        mats = [
            lines[(field * SLAB + i) * ROWS_Y : (field * SLAB + i + 1) * ROWS_Y]
            for i in range(SLAB)
            for field in range(2)
        ]
        for part, mat in enumerate(swap_groups(mats)):
            y_send[part] = mat

    def z_back(mats):
        lines = swap_groups(mats)
        stacked = jnp.concatenate([lines[2 * i + f] for f in range(2) for i in range(SLAB)], axis=0)
        values = times_table(stacked, bz)
        half = SLAB * ROWS_Y
        return values[:half], values[half:]

    def y_forward():
        both = table_times(ty, y_recv[...].reshape(CELLS, LANES))
        lines = both[:MODES] - turn(both[MODES:])
        x_send.reshape(MODES, LANES)[...] = lines

    def x_middle(x_recv, carried):
        rows = x_recv.reshape(CELLS, LANES)
        mats = [rows[pl.ds(ky, PLANE, stride=LINES_Y), :] for ky in range(LINES_Y)]
        lines = jnp.concatenate(swap_groups(mats), axis=0)
        both = table_times(tx, lines)
        cosine, sine = both[:MODES], both[MODES:]
        real, imag = factor[0], factor[1]
        first = (lane_index(cosine.shape) & 16) == 0
        spectrum, turned = cosine - turn(sine), turn(cosine) + sine
        if carried:
            spectrum, turned = spectrum + carry[0], turned + carry[1]
        rate = real * spectrum + imag * turned
        rate_turned = real * turned - imag * spectrum
        spectrum = factor[2] * roll(rate, 16) + spectrum
        turned = factor[2] * roll(rate_turned, 16) + turned
        rate = jnp.where(first, rate, real * spectrum + imag * turned)
        rate_turned = jnp.where(first, rate_turned, real * turned - imag * spectrum)
        if not carried:
            carry[0] = rate
            carry[1] = rate_turned
        lines = table_times(bx, jnp.concatenate([rate, rate_turned], axis=0))
        target = b_send.reshape(CELLS, LANES)
        mats = [lines[i * PLANE : (i + 1) * PLANE] for i in range(SLAB)]
        for ky, mat in enumerate(swap_groups(mats)):
            target[pl.ds(ky, PLANE, stride=LINES_Y), :] = mat

    def prepare_carry():
        first = (lane_index((MODES, LANES)) & 16) == 0
        for i in range(2):
            carry[i] = jnp.where(first, factor[2] * roll(carry[i], -16), 0.0)

    def y_back():
        lines = b_recv.reshape(MODES, LANES)[...]
        cells = table_times(by, jnp.concatenate([lines, turn(lines)], axis=0))
        u_send[...] = cells.reshape(PARTS_Y, ROWS_Y, LANES)

    for i in range(3):
        loads[i].wait()
    start = v[...].reshape(SLAB * ROWS_Y, CELLS)
    react = r[...].reshape(SLAB * ROWS_Y, CELLS)
    z_forward(start, react * start)
    for i in range(3, 8):
        loads[i].wait()
    pl.semaphore_wait(barrier, heard)
    for dy in (3, 0):
        for dz in (4, RING_Z - 4):
            pl.semaphore_signal(
                ready, inc=1, device_id=plane_id(*place(dy, dz)), device_id_type=MESH
            )

    others_y = pl.ds(0, PARTS_Y - 1)
    others_x = pl.ds(0, PLANE - 1)
    others_b = pl.ds(0, PAIRS - 1)
    y_exchange(y_send, y_recv, Y_OUT)
    prepare_factor()
    received(y_recv.at[others_y], Y_OUT)
    y_forward()
    pl.semaphore_wait(ready, 4)
    x_exchange(x_recv1, X_OUT)
    received(x_recv1.at[others_x], X_OUT)
    x_middle(x_recv1, False)
    x_return(X_BACK, 0)
    prepare_carry()
    received(b_recv.at[others_b], X_BACK)
    y_back()
    sent(y_send.at[others_y], Y_OUT)
    y_exchange(u_send, u_recv, Y_BACK)
    received(u_recv.at[others_y], Y_BACK)
    smooth, smooth_rate = z_back([u_recv[part] for part in range(PARTS_Y)])
    rate1 = smooth + react * start
    rate2 = smooth_rate + react * rate1
    z_forward(react * rate1, react * rate2)

    sent(x_recv1.at[others_x], X_OUT)
    sent(b_send.at[others_b], X_BACK)
    y_exchange(y_send, y_recv, Y_OUT2)
    known = start + rate1
    piece_send[0] = known.reshape(SLAB, ROWS_Y, CELLS)
    known = known + 0.5 * rate2
    piece_send[1] = known.reshape(SLAB, ROWS_Y, CELLS)
    known = known + 0.25 * (react * rate2)
    piece_send[2] = known.reshape(SLAB, ROWS_Y, CELLS)
    known = known + 0.125 * (react * (react * rate2))
    piece_send[3] = known.reshape(SLAB, ROWS_Y, CELLS)

    def send_pieces(point):
        for level in range(LEVELS):
            cuts = (0, *CUTS[level // 2])

            @pl.when(lvl != level)
            def _(level=level, cuts=cuts):
                for at in range(cuts[point], cuts[point + 1]):
                    half = pl.ds(at % 2 * (ROWS_Y // 2), ROWS_Y // 2)
                    source = piece_send.at[level, at // 2, half]
                    target = piece.at[lvl * SLAB + at // 2, half]
                    remote(source, target, BULK, {"lvl": level}).start()

    send_pieces(0)
    piece[own] = piece_send[lvl]

    received(y_recv.at[others_y], Y_OUT2)
    y_forward()
    x_exchange(x_recv2, X_OUT2)
    send_pieces(1)
    received(x_recv2.at[others_x], X_OUT2)
    x_middle(x_recv2, True)
    x_return(X_BACK2, 1)
    send_pieces(2)
    received(b_recv.at[others_b], X_BACK2)
    sent(u_send.at[others_y], Y_BACK)
    y_back()

    before = lax.rem(at_z + RING_Z - 1, RING_Z)
    slab, block = lax.rem(before, 4), row_y * 4 + lax.div(before, 4)

    def last(level, k):
        other = lax.rem(gy + k, PARTS_Y)
        remote(
            u_send.at[other],
            f_recv.at[slab, gy],
            FINAL + slab,
            {"lvl": level, "gx": block, "gy": other},
            FINAL + level,
        ).start()

    for k in (4, 3, 5, 2, 6, 1, 7):
        for level in (3, 2):
            last(level, k)
    for level in (3, 2):
        @pl.when(lvl != level)
        def _(level=level):
            last(level, 0)

        @pl.when(lvl == level)
        def _():
            f_recv[slab, gy] = u_send[gy]

    send_pieces(3)
    loads[8].wait()
    received(piece.at[pl.ds(0, ROWS_X - SLAB)], BULK)

    @pl.when(lvl >= 2)
    def _():
        last_weight = jnp.where(lvl == 3, 0.125, 0.0)
        def add(steps):
            slabs = [lax.rem(lvl - 1 + step, LEVELS) for step in steps]
            for t, step in zip(slabs, steps):
                received(f_recv.at[t] if step else f_recv.at[t, others_y], FINAL + t)
            parts = [z_back([f_recv[t, part] for part in range(PARTS_Y)]) for t in slabs]
            for t, (first, second) in zip(slabs, parts):
                at = pl.ds(t * SLAB, SLAB)
                first = first.reshape(SLAB, ROWS_Y, CELLS)
                second = second.reshape(SLAB, ROWS_Y, CELLS)
                scale = 0.25 + last_weight * r_all[at]
                piece[at] = piece[at] + scale * first + last_weight * second

        add((0,))
        add((3, 1, 2))

    sent(y_send.at[others_y], Y_OUT2)
    sent(x_recv2.at[others_x], X_OUT2)
    sent(b_send.at[others_b], X_BACK2)
    sent(piece_send.at[pl.ds(0, 3)], BULK)
    for level in (3, 2):
        @pl.when(lvl != level)
        def _(level=level):
            sent(u_send, FINAL + level)

        @pl.when(lvl == level)
        def _(level=level):
            sent(u_send.at[others_y], FINAL + level)


def solution(mesh):
    constants = tables()

    def shards(initial, reaction):
        rows = (SLAB, ROWS_Y, CELLS)
        block = (ROWS_X, ROWS_Y, CELLS)
        lines = (PARTS_Y, ROWS_Y, LANES)
        chunks = (PLANE, LINES_Y, LANES)
        half_chunks = (PAIRS, LINES_Y, LANES)
        vmem = pltpu.VMEM
        result = pl.pallas_call(
            kernel,
            out_shape=pltpu.VMEM(block, F32),
            in_specs=[pl.BlockSpec(memory_space=pl.ANY)] * 8,
            out_specs=pl.BlockSpec(memory_space=pltpu.VMEM),
            scratch_shapes=[
                vmem(rows, F32),
                vmem(rows, F32),
                vmem(block, F32),
                *[vmem(t.shape, BF16) for t in constants],
                vmem((3, MODES, LANES), F32),
                vmem((2, MODES, LANES), F32),
                vmem(lines, F32),
                vmem(lines, F32),
                vmem(half_chunks, F32),
                vmem(chunks, F32),
                vmem(chunks, F32),
                vmem(chunks, F32),
                vmem(half_chunks, F32),
                vmem(lines, F32),
                vmem(lines, F32),
                vmem((LEVELS, *lines), F32),
                vmem((LEVELS, *rows), F32),
                pltpu.SemaphoreType.DMA((9,)),
                pltpu.SemaphoreType.DMA((PHASES,)),
                pltpu.SemaphoreType.DMA((PHASES,)),
                pltpu.SemaphoreType.REGULAR,
            ],
            compiler_params=pltpu.CompilerParams(collective_id=0, has_side_effects=True),
        )(initial, reaction, *[jnp.asarray(t) for t in constants])
        return result[None]

    in_specs = (P("gx", "gy", None), P("gx", "gy", None))
    out_specs = P("lvl", "gx", "gy", None)
    return jax.shard_map(shards, mesh=mesh, in_specs=in_specs, out_specs=out_specs, check_vma=False)
```
